32 devices in a mesh: genome: 8 (over z, x), samples: 4 (over y, core).
Axes of the slice: x: 2, y: 2, z: 4, core: 2. Of those that a mesh axis runs over, the one named last changes fastest.
Arguments:
- genotypes: int32 [4096, 12288], P('samples', 'genome'), may hold values from 0 to 2
- residuals: bfloat16 [4096, 64], P('samples'), may hold values from -78 to 78
- variant_class: int32 [12288], P('genome'), may hold values from 0 to 7
- class_weight: float32 [8], replicated, may hold values from 0.25 to 4
- gene_start: int32 [512], P(('genome', 'samples')), may hold values from 0 to 12287, as said below
- gene_end: int32 [512], P(('genome', 'samples')), may hold values from 1 to 12288, as said below
Outputs:
- score_track: float32 [12288, 64], P(('genome', 'samples'))
- gene_stat: float32 [512, 64], P(('genome', 'samples'))
The draws below stay inside these ranges and needn't reach their ends.
Inputs may be any that keep to these rules, and one draw needn't show every extreme that they name: gene_end[g] - 1 lies in [k * 384, (k + 1) * 384) with k = g // 16. 1 <= gene_end[g] - gene_start[g] <= 384.
All inputs are finite; a program needn't handle non-finite values.
Results may differ from the reference program's by a relative error of at most 0.0003.
Values sent between devices are 32-bit elements; how exact they have to be, the bound alone decides.
No kernel may reach another device: no remote copies, remote signals or barrier semaphores. Data moves between devices by JAX's collectives and lax.ppermute only.
A program may use at most 64 MiB of HBM per device.

```python
import math
import jax
import jax.numpy as jnp
from jax import lax

PHENO = 64
CLASSES = 8
S_DEV = 1024
GENE_DEV = 16
SAMPLES = 4096
VARIANTS = 12288
GENES = 512
N_SAMPLES = 4


def log_uniform(key, shape, lower, upper):
    return jnp.exp(jax.random.uniform(key, shape, jnp.float32, math.log(lower), math.log(upper)))


def draw_genotypes(key, part):
    key_rate, key_first, key_second = jax.random.split(jax.random.fold_in(key, 11), 3)
    base_rate = jax.random.randint(key_rate, (VARIANTS,), 1, 8)
    rising = 7 * jnp.arange(VARIANTS, dtype=jnp.int32) // VARIANTS
    allele_rate = (base_rate + rising)[None, :]
    first_draw = jax.random.randint(key_first, (SAMPLES, VARIANTS), 0, 16)
    second_draw = jax.random.randint(key_second, (SAMPLES, VARIANTS), 0, 16)
    return ((first_draw < allele_rate).astype(jnp.int32) + (second_draw < allele_rate).astype(jnp.int32)).astype(jnp.int32)


def draw_residuals(key, part):
    key_noise, key_rows, key_cols = jax.random.split(jax.random.fold_in(key, 23), 3)
    position = jnp.arange(SAMPLES, dtype=jnp.float32) / SAMPLES
    trend = jnp.sqrt(1.0 + 2.0 * position)
    noise = jnp.clip(jax.random.normal(key_noise, (SAMPLES, PHENO), jnp.float32), -5.0, 5.0)
    row_scale = log_uniform(key_rows, (SAMPLES,), 0.3, 3.0) * trend
    col_scale = log_uniform(key_cols, (PHENO,), 0.3, 3.0)
    return (noise * row_scale[:, None] * col_scale[None, :]).astype(jnp.bfloat16)


def gene_bounds(key):
    key_last, key_length = jax.random.split(jax.random.fold_in(key, 37), 2)
    genes_index = jnp.arange(GENES, dtype=jnp.int32)
    block_index = genes_index // GENE_DEV
    block_size = VARIANTS // (GENES // GENE_DEV)
    last_variant = block_index * block_size + jax.random.randint(key_last, (GENES,), 0, block_size)
    window_length = jax.random.randint(key_length, (GENES,), 1, block_size + 1)
    end_index = last_variant + 1
    start_index = jnp.maximum(end_index - window_length, 0)
    return (start_index.astype(jnp.int32), end_index.astype(jnp.int32))


def draw_gene_start(key, part):
    return gene_bounds(key)[0]


def draw_gene_end(key, part):
    return gene_bounds(key)[1]


def place_ends(drawn, stream_key, low, top_value):
    longest = drawn.shape.index(max(drawn.shape))
    spots = []
    for shift in (0, 1):
        where = [jax.random.randint(jax.random.fold_in(stream_key, axis), (), 0, length) for axis, length in enumerate(drawn.shape)]
        where[longest] = (where[longest] + shift) % drawn.shape[longest]
        spots.append(tuple(where))
    return drawn.at[spots[0]].set(low).at[spots[1]].set(top_value)


def setup_inputs(seed: int = 0) -> dict:
    key_list = jax.random.split(jax.random.key(seed), 7)
    genotypes = draw_genotypes(jax.random.fold_in(key_list[6], 71), 0)
    residuals = draw_residuals(jax.random.fold_in(key_list[6], 71), 0)
    variant_class = place_ends(jax.random.randint(key_list[2], (VARIANTS,), 0, CLASSES), jax.random.fold_in(key_list[2], 1), 0, CLASSES - 1).astype(jnp.int32)
    class_weight = jnp.clip(jnp.exp(jax.random.uniform(key_list[3], (CLASSES,), jnp.float32, math.log(0.25), math.log(4.0))), 0.25, 4.0)
    gene_start = draw_gene_start(jax.random.fold_in(key_list[6], 71), 0)
    gene_end = draw_gene_end(jax.random.fold_in(key_list[6], 71), 0)
    return dict(genotypes=genotypes, residuals=residuals, variant_class=variant_class, class_weight=class_weight, gene_start=gene_start, gene_end=gene_end)


def reference(genotypes, residuals, variant_class, class_weight, gene_start, gene_end):
    contract = (((0,), (0,)), ((), ()))

    def add_block(block_index, carry):
        partial_value, squared = carry
        offset = (block_index * S_DEV).astype(jnp.int32)
        sample_block = lax.dynamic_slice_in_dim(genotypes, offset, S_DEV, 0).astype(jnp.bfloat16)
        residual_block = lax.dynamic_slice_in_dim(residuals, offset, S_DEV, 0)
        partial_value = partial_value + lax.dot_general(sample_block, residual_block, contract, preferred_element_type=jnp.float32)
        squared = squared + lax.dot_general(sample_block * sample_block, jnp.ones((S_DEV,), jnp.bfloat16), contract, preferred_element_type=jnp.float32)
        return (partial_value, squared)

    start_sums = (jnp.zeros((VARIANTS, PHENO), jnp.float32), jnp.zeros((VARIANTS,), jnp.float32))
    partial_value, counts = lax.fori_loop(0, N_SAMPLES, add_block, start_sums)
    weight = class_weight[variant_class]
    scores = partial_value * weight[:, None] * (SAMPLES ** -0.5)
    quad_terms = weight * weight * counts / SAMPLES
    spread = jnp.sum(jnp.square(residuals.astype(jnp.float32)), axis=0) / SAMPLES + 1e-5
    prefix = jnp.cumsum(scores, axis=0)
    quad_prefix = jnp.cumsum(quad_terms)
    score_track = prefix * (VARIANTS ** -0.5)
    padded = jnp.concatenate([jnp.zeros((1, PHENO), jnp.float32), prefix], axis=0)
    quad_padded = jnp.concatenate([jnp.zeros((1,), jnp.float32), quad_prefix], axis=0)
    gene_score = padded[gene_end] - padded[gene_start]
    gene_quad = quad_padded[gene_end] - quad_padded[gene_start]
    gene_stat = jnp.square(gene_score) / (spread[None, :] * (gene_quad[:, None] + 1.0))
    return (score_track, gene_stat)
```

```python
import jax
import jax.numpy as jnp
from jax import lax
from jax.experimental import pallas as pl
from jax.experimental.pallas import tpu as pltpu
from jax.sharding import PartitionSpec as P

F32, BF16 = jnp.float32, jnp.bfloat16
TN = (((0,), (0,)), ((), ()))
NT = (((1,), (1,)), ((), ()))
NN = (((1,), (0,)), ((), ()))
LANES = 128
SUBLANES = 8
VMEM_LIMIT = 16 * 2**20


def rounded(size, unit):
    return (size + unit - 1) // unit * unit


def visit_order(groups):
    masks, bit = [0], groups // 2
    while bit:
        masks = [mask | bit for mask in masks] + masks
        bit //= 2
    return masks


def split(x):
    high = x.astype(BF16)
    rest = x - high.astype(F32)
    middle = rest.astype(BF16)
    return high, middle, (rest - middle.astype(F32)).astype(BF16)


def exact_dot(a, b, dims):
    return sum(lax.dot_general(a, part, dims, preferred_element_type=F32) for part in split(b))


def exact_dot_left(a, b, dims):
    return sum(lax.dot_general(part, b, dims, preferred_element_type=F32) for part in split(a))


def first_kernel(total_samples, groups):
    def body(class_weight, genotypes, residuals, classes, send, keep, buffer, sems):
        phenos, rows = residuals.shape
        share = send.shape[2]
        me = lax.axis_index("samples")
        extra = send.shape[1] - phenos
        order = [me ^ mask for mask in visit_order(groups)]

        def copy(step):
            start = pl.multiple_of(order[step] * share, LANES)
            return pltpu.make_async_copy(
                genotypes.at[:, pl.ds(start, share)], buffer.at[step], sems.at[step]
            )

        for step in range(groups):
            copy(step).start()
        res = residuals[...]
        res32 = res.astype(F32)
        ones = jnp.ones((extra, rows), BF16)
        row_of = lax.broadcasted_iota(jnp.int32, (extra, LANES), 0)
        spread = exact_dot(ones, jnp.square(res32), NT)
        small = jnp.where(
            row_of == groups + 1,
            jnp.concatenate([spread, jnp.zeros((extra, LANES - phenos), F32)], axis=1),
            0.0,
        )
        mark_rows = lax.broadcasted_iota(jnp.int32, (extra, share), 0)
        for step in range(groups):
            copy(step).wait()
            dosage = buffer[step].astype(F32)
            part = lax.dot_general(
                res, dosage.astype(BF16), NN, preferred_element_type=F32
            )
            counts = jnp.sum(dosage * dosage, axis=0, keepdims=True)
            kind = classes[:, pl.ds(pl.multiple_of(order[step] * share, LANES), share)]
            weight = jnp.zeros((1, share), F32)
            for c in range(class_weight.shape[0]):
                weight = jnp.where(kind == c, class_weight[c], weight)
            scores = part * (weight * total_samples ** (-0.5))
            quad = weight * weight * counts / total_samples
            out = send if step < groups // 2 else keep
            slot = step % (groups // 2)
            out[slot, :phenos, :] = scores
            out[slot, phenos:, :] = jnp.where(mark_rows == 0, quad, 0.0)
            both = jnp.concatenate(
                [scores, jnp.broadcast_to(quad, (LANES - phenos, share))], axis=0
            )
            mark = (mark_rows == order[step] + 1).astype(F32).astype(BF16)
            small = small + exact_dot(mark, both, NT)
        for out in (send, keep):
            head = out[0, phenos:, :LANES]
            out[0, phenos:, :LANES] = jnp.where(row_of == 0, head, small)

    return body


def first_variant(real_share):
    groups = lax.axis_size("samples")
    return (lax.axis_index("genome") * groups + lax.axis_index("samples")) * real_share


def second_kernel(groups, real_share):
    def body(start_ref, end_ref, pair, received, fin, prefix, totals, own_genes):
        phenos = prefix.shape[0]
        share = prefix.shape[1]
        genes = own_genes.shape[0]
        me = lax.axis_index("samples")
        extra = totals.shape[0]
        block = pair[1] + received[...]
        fin[...] = block
        small = pair[0, phenos:, :LANES] + received[phenos:, :LANES]
        rows = lax.broadcasted_iota(jnp.int32, (share, share), 0)
        cols = lax.broadcasted_iota(jnp.int32, (share, share), 1)
        upper = (rows <= cols).astype(F32).astype(BF16)
        scores = block[:phenos]
        prefix[...] = exact_dot_left(scores, upper, NN)
        row_of = lax.broadcasted_iota(jnp.int32, (extra, LANES), 0)
        is_total = (row_of >= 1) & (row_of <= groups)
        whole = jnp.sum(jnp.where(is_total, small, 0.0), axis=0, keepdims=True)
        before = jnp.sum(
            jnp.where(is_total & (row_of < me + 1), small, 0.0), axis=0, keepdims=True
        )
        spread = jnp.sum(jnp.where(row_of == groups + 1, small, 0.0), axis=0, keepdims=True)
        totals[...] = jnp.where(
            row_of == 0, whole, jnp.where(row_of == 1, before, jnp.where(row_of == 2, spread, 0.0))
        )
        own_genes[...] = gene_sums(start_ref, end_ref, first_variant(real_share), block, genes)

    return body


def gene_sums(start_ref, end_ref, base, block, genes):
    share = block.shape[1]
    index = lax.broadcasted_iota(jnp.int32, (genes, 1), 0)
    start = jnp.zeros((genes, 1), jnp.int32)
    end = jnp.zeros((genes, 1), jnp.int32)
    for g in range(genes):
        start = jnp.where(index == g, start_ref[g] - base, start)
        end = jnp.where(index == g, end_ref[g] - base, end)
    spot = lax.broadcasted_iota(jnp.int32, (genes, share), 1)
    inside = ((spot >= start) & (spot < end)).astype(F32).astype(BF16)
    return exact_dot(inside, block, NT)


def third_kernel(total_samples, total_vars, real_share):
    def body(start_ref, end_ref, prefix, carry, totals, earlier, own_genes, track, stat):
        phenos, share = prefix.shape
        genes = own_genes.shape[0]
        row_of = lax.broadcasted_iota(jnp.int32, totals.shape, 0)
        rows = totals[...]
        base = jnp.where(row_of == 0, carry[0:1, :], jnp.where(row_of == 1, rows, 0.0))
        ones = jnp.where(
            lax.broadcasted_iota(jnp.int32, (rows.shape[0], share), 0) < 2, 1.0, 0.0
        ).astype(BF16)
        lifted = exact_dot_left(base, ones, TN)[:phenos]
        track[...] = (prefix[...] + lifted) * total_vars ** (-0.5)
        sums = own_genes[...] + gene_sums(
            start_ref, end_ref, first_variant(real_share) - real_share, earlier[...], genes
        )
        variance = rows[2:3, :phenos] / total_samples + 1e-05
        quad = sums[:, phenos : phenos + 1]
        stat[...] = jnp.square(sums[:, :phenos]) / (variance * (quad + 1.0))

    return body


def call(body, name, ins, outs, final=False, **more):
    spaces = {"s": pltpu.SMEM, "v": pltpu.VMEM, "h": pltpu.HBM}
    args = [
        x if kind == "s" else pltpu.with_memory_space_constraint(x, spaces[kind])
        for kind, x in ins
    ]
    result = jax.ShapeDtypeStruct if final else pltpu.VMEM
    return pl.pallas_call(
        body,
        in_specs=[pl.BlockSpec(memory_space=spaces[kind]) for kind, _ in ins],
        out_specs=[pl.BlockSpec(memory_space=pltpu.VMEM)] * len(outs),
        out_shape=[result(shape, F32) for shape in outs],
        compiler_params=pltpu.CompilerParams(vmem_limit_bytes=VMEM_LIMIT),
        name=name,
        **more,
    )(*args)


def local(genotypes, residuals, variant_class, class_weight, gene_start, gene_end):
    groups = lax.axis_size("samples")
    blocks = lax.axis_size("genome")
    both_axes = ("genome", "samples")
    sample_rows, block_vars = genotypes.shape
    phenos = residuals.shape[1]
    genes = gene_start.shape[0]
    real_share = block_vars // groups
    share = rounded(real_share, LANES)
    total_samples = sample_rows * groups
    total_vars = block_vars * blocks
    block_index = lax.axis_index("genome").astype(jnp.int32)
    extra = rounded(groups + 2, SUBLANES)
    rows = phenos + extra
    half = groups // 2
    classes = variant_class.reshape(1, block_vars)
    if share != real_share:
        missing = share - real_share
        classes = jnp.pad(variant_class.reshape(groups, real_share), ((0, 0), (0, missing)))
        classes = classes.reshape(1, groups * share)
        genotypes = jnp.pad(
            genotypes.reshape(sample_rows, groups, real_share), ((0, 0), (0, 0), (0, missing))
        ).reshape(sample_rows, groups * share)

    send, keep = call(
        first_kernel(total_samples, groups),
        "first",
        [("s", class_weight), ("h", genotypes), ("v", residuals.T), ("v", classes)],
        [(half, rows, share)] * 2,
        scratch_shapes=[
            pltpu.VMEM((groups, sample_rows, share), jnp.int32),
            pltpu.SemaphoreType.DMA((groups,)),
        ],
    )

    bit = 1
    pair = keep + lax.ppermute(send, "samples", [(i, i ^ bit) for i in range(groups)])
    while half > 2:
        bit, half = 2 * bit, half // 2
        small = jnp.pad(
            pair[:1, phenos + 1 :, :LANES], ((0, half - 1), (phenos + 1, 0), (0, share - LANES))
        )
        other = lax.ppermute(pair[:half], "samples", [(i, i ^ bit) for i in range(groups)])
        pair = pair[half:] + other + small
    bit *= 2
    received = lax.ppermute(pair[0], "samples", [(i, i ^ bit) for i in range(groups)])

    fin, prefix, totals, own_genes = call(
        second_kernel(groups, real_share),
        "second",
        [("s", gene_start), ("s", gene_end), ("v", pair), ("v", received)],
        [(rows, share), (phenos, share), (extra, LANES), (genes, rows)],
    )

    last = groups * blocks
    even = lax.ppermute(fin, both_axes, [(k, k + 1) for k in range(0, last, 2)])
    odd = lax.ppermute(fin, both_axes, [(k, k + 1) for k in range(1, last - 1, 2)])
    whole = totals[:1]
    carry = jnp.zeros_like(whole)
    bit = 1
    while bit < blocks:
        one_way = 2 * bit >= blocks
        pairs = [(k, k ^ bit) for k in range(blocks) if not (one_way and k & bit)]
        other = lax.ppermute(whole, "genome", pairs)
        carry = carry + jnp.where((block_index & bit) != 0, other, 0.0)
        whole = whole + other
        bit *= 2

    track, stat = call(
        third_kernel(total_samples, total_vars, real_share),
        "third",
        [("s", gene_start), ("s", gene_end)]
        + [("v", x) for x in (prefix, carry, totals, even + odd, own_genes)],
        [(phenos, share), (genes, phenos)],
        final=True,
    )
    return track[:, :real_share].T, stat


def solution(mesh):
    return jax.shard_map(
        local,
        mesh=mesh,
        in_specs=(
            P("samples", "genome"),
            P("samples", None),
            P("genome"),
            P(),
            P(("genome", "samples")),
            P(("genome", "samples")),
        ),
        out_specs=(P(("genome", "samples"), None), P(("genome", "samples"), None)),
        check_vma=False,
    )
```

```python
import jax
import jax.numpy as jnp
from jax import lax
from jax.experimental import pallas as pl
from jax.experimental.pallas import tpu as pltpu
from jax.sharding import PartitionSpec as P

F32, BF16 = jnp.float32, jnp.bfloat16
TN = (((0,), (0,)), ((), ()))
NT = (((1,), (1,)), ((), ()))
NN = (((1,), (0,)), ((), ()))
LANES = 128
SUBLANES = 8
VMEM_LIMIT = 16 * 2**20


def rounded(size, unit):
    return (size + unit - 1) // unit * unit


def visit_order(groups):
    masks, bit = [0], groups // 2
    while bit:
        masks = [mask | bit for mask in masks] + masks
        bit //= 2
    return masks


def split(x):
    high = x.astype(BF16)
    rest = x - high.astype(F32)
    middle = rest.astype(BF16)
    return high, middle, (rest - middle.astype(F32)).astype(BF16)


def exact_dot(a, b, dims):
    return sum(lax.dot_general(a, part, dims, preferred_element_type=F32) for part in split(b))


def exact_dot_left(a, b, dims):
    return sum(lax.dot_general(part, b, dims, preferred_element_type=F32) for part in split(a))


def first_kernel(total_samples, groups):
    def body(
        weight_hbm, genotypes, residuals_hbm, classes_hbm, send, keep,
        buffer, sems, class_weight, residuals, classes, small_sems,
    ):
        phenos, rows = residuals.shape
        share = send.shape[2]
        me = lax.axis_index("samples")
        extra = send.shape[1] - phenos
        order = [me ^ mask for mask in visit_order(groups)]

        def copy(step):
            start = pl.multiple_of(order[step] * share, LANES)
            return pltpu.make_async_copy(
                genotypes.at[:, pl.ds(start, share)], buffer.at[step], sems.at[step]
            )

        small_copies = [
            pltpu.make_async_copy(source, target, small_sems.at[k])
            for k, (source, target) in enumerate(
                [(residuals_hbm, residuals), (classes_hbm, classes), (weight_hbm, class_weight)]
            )
        ]
        for each in small_copies:
            each.start()
        for step in range(groups):
            copy(step).start()
        for each in small_copies:
            each.wait()
        res = residuals[...]
        res32 = res.astype(F32)
        ones = jnp.ones((extra, rows), BF16)
        row_of = lax.broadcasted_iota(jnp.int32, (extra, LANES), 0)
        spread = exact_dot(ones, jnp.square(res32), NT)
        small = jnp.where(
            row_of == groups + 1,
            jnp.concatenate([spread, jnp.zeros((extra, LANES - phenos), F32)], axis=1),
            0.0,
        )
        mark_rows = lax.broadcasted_iota(jnp.int32, (extra, share), 0)
        for step in range(groups):
            copy(step).wait()
            dosage = buffer[step].astype(F32)
            part = lax.dot_general(
                res, dosage.astype(BF16), NN, preferred_element_type=F32
            )
            counts = jnp.sum(dosage * dosage, axis=0, keepdims=True)
            kind = classes[pl.ds(pl.multiple_of(order[step] * share, LANES), share)].reshape(1, share)
            weight = jnp.zeros((1, share), F32)
            for c in range(class_weight.shape[0]):
                weight = jnp.where(kind == c, class_weight[c], weight)
            scores = part * (weight * total_samples ** (-0.5))
            quad = weight * weight * counts / total_samples
            out = send if step < groups // 2 else keep
            slot = step % (groups // 2)
            out[slot, :phenos, :] = scores
            out[slot, phenos:, :] = jnp.where(mark_rows == 0, quad, 0.0)
            both = jnp.concatenate(
                [scores, jnp.broadcast_to(quad, (LANES - phenos, share))], axis=0
            )
            mark = (mark_rows == order[step] + 1).astype(F32).astype(BF16)
            small = small + exact_dot(mark, both, NT)
        for out in (send, keep):
            head = out[0, phenos:, :LANES]
            out[0, phenos:, :LANES] = jnp.where(row_of == 0, head, small)

    return body


def first_variant(real_share):
    groups = lax.axis_size("samples")
    return (lax.axis_index("genome") * groups + lax.axis_index("samples")) * real_share


def second_kernel(groups, real_share):
    def body(start_ref, end_ref, pair, received, fin, prefix, totals, own_genes):
        phenos = prefix.shape[0]
        share = prefix.shape[1]
        genes = own_genes.shape[0]
        me = lax.axis_index("samples")
        extra = totals.shape[0]
        block = pair[1] + received[...]
        fin[...] = block
        small = pair[0, phenos:, :LANES] + received[phenos:, :LANES]
        rows = lax.broadcasted_iota(jnp.int32, (share, share), 0)
        cols = lax.broadcasted_iota(jnp.int32, (share, share), 1)
        upper = (rows <= cols).astype(F32).astype(BF16)
        scores = block[:phenos]
        prefix[...] = exact_dot_left(scores, upper, NN)
        row_of = lax.broadcasted_iota(jnp.int32, (extra, LANES), 0)
        is_total = (row_of >= 1) & (row_of <= groups)
        whole = jnp.sum(jnp.where(is_total, small, 0.0), axis=0, keepdims=True)
        before = jnp.sum(
            jnp.where(is_total & (row_of < me + 1), small, 0.0), axis=0, keepdims=True
        )
        spread = jnp.sum(jnp.where(row_of == groups + 1, small, 0.0), axis=0, keepdims=True)
        totals[...] = jnp.where(
            row_of == 0, whole, jnp.where(row_of == 1, before, jnp.where(row_of == 2, spread, 0.0))
        )
        own_genes[...] = gene_sums(start_ref, end_ref, first_variant(real_share), block, genes)

    return body


def gene_sums(start_ref, end_ref, base, block, genes):
    share = block.shape[1]
    index = lax.broadcasted_iota(jnp.int32, (genes, 1), 0)
    start = jnp.zeros((genes, 1), jnp.int32)
    end = jnp.zeros((genes, 1), jnp.int32)
    for g in range(genes):
        start = jnp.where(index == g, start_ref[g] - base, start)
        end = jnp.where(index == g, end_ref[g] - base, end)
    spot = lax.broadcasted_iota(jnp.int32, (genes, share), 1)
    inside = ((spot >= start) & (spot < end)).astype(F32).astype(BF16)
    return exact_dot(inside, block, NT)


def third_kernel(total_samples, total_vars, real_share):
    def body(start_ref, end_ref, prefix, carry, totals, near, far, own_genes, track, stat):
        phenos, share = prefix.shape
        genes = own_genes.shape[0]
        row_of = lax.broadcasted_iota(jnp.int32, totals.shape, 0)
        rows = totals[...]
        base = jnp.where(row_of == 0, carry[0:1, :], jnp.where(row_of == 1, rows, 0.0))
        ones = jnp.where(
            lax.broadcasted_iota(jnp.int32, (rows.shape[0], share), 0) < 2, 1.0, 0.0
        ).astype(BF16)
        lifted = exact_dot_left(base, ones, TN)[:phenos]
        track[...] = (prefix[...] + lifted) * total_vars ** (-0.5)
        odd = lax.axis_index("samples") % 2 == 1
        earlier = jnp.where(odd, near[...], far[...])
        sums = own_genes[...] + gene_sums(
            start_ref, end_ref, first_variant(real_share) - real_share, earlier, genes
        )
        variance = rows[2:3, :phenos] / total_samples + 1e-05
        quad = sums[:, phenos : phenos + 1]
        stat[...] = jnp.square(sums[:, :phenos]) / (variance * (quad + 1.0))

    return body


def call(body, name, ins, outs, final=False, **more):
    spaces = {"s": pltpu.SMEM, "v": pltpu.VMEM, "h": pltpu.HBM}
    args = [
        x if kind == "s" else pltpu.with_memory_space_constraint(x, spaces[kind])
        for kind, x in ins
    ]
    result = jax.ShapeDtypeStruct if final else pltpu.VMEM
    return pl.pallas_call(
        body,
        in_specs=[pl.BlockSpec(memory_space=spaces[kind]) for kind, _ in ins],
        out_specs=[pl.BlockSpec(memory_space=pltpu.VMEM)] * len(outs),
        out_shape=[result(shape, F32) for shape in outs],
        compiler_params=pltpu.CompilerParams(vmem_limit_bytes=VMEM_LIMIT),
        name=name,
        **more,
    )(*args)


def block_prefix(whole, blocks, groups):
    devices = blocks * groups
    index = lax.axis_index("genome")
    both_axes = ("genome", "samples")

    def exchange(x, mask):
        return lax.ppermute(x, both_axes, [(k, k ^ mask ^ 1) for k in range(devices)])

    carry = jnp.zeros_like(whole)
    bit = 1
    while bit < blocks:
        other = exchange(whole, bit * groups)
        carry = carry + jnp.where((index & bit) != 0, other, 0.0)
        whole = whole + other
        bit *= 2
    bit = 2
    while bit < groups:
        carry = carry + exchange(carry, bit)
        bit *= 2
    return carry


def local(genotypes, residuals, variant_class, class_weight, gene_start, gene_end):
    groups = lax.axis_size("samples")
    blocks = lax.axis_size("genome")
    both_axes = ("genome", "samples")
    sample_rows, block_vars = genotypes.shape
    phenos = residuals.shape[1]
    genes = gene_start.shape[0]
    real_share = block_vars // groups
    share = rounded(real_share, LANES)
    total_samples = sample_rows * groups
    total_vars = block_vars * blocks
    extra = rounded(groups + 2, SUBLANES)
    rows = phenos + extra
    devices = groups * blocks
    half = groups // 2
    classes = variant_class
    if share != real_share:
        missing = share - real_share
        classes = jnp.pad(variant_class.reshape(groups, real_share), ((0, 0), (0, missing)))
        classes = classes.reshape(groups * share)
        genotypes = jnp.pad(
            genotypes.reshape(sample_rows, groups, real_share), ((0, 0), (0, 0), (0, missing))
        ).reshape(sample_rows, groups * share)

    send, keep = call(
        first_kernel(total_samples, groups),
        "first",
        [("h", class_weight), ("h", genotypes), ("h", residuals.T), ("h", classes)],
        [(half, rows, share)] * 2,
        scratch_shapes=[
            pltpu.VMEM((groups, sample_rows, share), jnp.int32),
            pltpu.SemaphoreType.DMA((groups,)),
            pltpu.SMEM(class_weight.shape, F32),
            pltpu.VMEM((phenos, sample_rows), BF16),
            pltpu.VMEM((groups * share,), jnp.int32),
            pltpu.SemaphoreType.DMA((3,)),
        ],
    )

    bit = 1
    pair = keep + lax.ppermute(send, "samples", [(i, i ^ bit) for i in range(groups)])
    while half > 2:
        bit, half = 2 * bit, half // 2
        small = jnp.pad(
            pair[:1, phenos + 1 :, :LANES], ((0, half - 1), (phenos + 1, 0), (0, share - LANES))
        )
        other = lax.ppermute(pair[:half], "samples", [(i, i ^ bit) for i in range(groups)])
        pair = pair[half:] + other + small
    whole = jnp.sum(pair[0, phenos + 1 : phenos + 1 + groups, :LANES], axis=0, keepdims=True)
    carry = block_prefix(whole, blocks, groups)
    bit *= 2
    received = lax.ppermute(pair[0], "samples", [(i, i ^ bit) for i in range(groups)])

    fin, prefix, totals, own_genes = call(
        second_kernel(groups, real_share),
        "second",
        [("s", gene_start), ("s", gene_end), ("v", pair), ("v", received)],
        [(rows, share), (phenos, share), (extra, LANES), (genes, rows)],
    )

    near = lax.ppermute(fin, both_axes, [(k, k ^ 1) for k in range(devices)])
    far = lax.ppermute(fin, both_axes, [(k, k + 1) for k in range(1, devices - 1, 2)])

    track, stat = call(
        third_kernel(total_samples, total_vars, real_share),
        "third",
        [("s", gene_start), ("s", gene_end)]
        + [("v", x) for x in (prefix, carry, totals, near, far, own_genes)],
        [(phenos, share), (genes, phenos)],
        final=True,
    )
    return track[:, :real_share].T, stat


def solution(mesh):
    return jax.shard_map(
        local,
        mesh=mesh,
        in_specs=(
            P("samples", "genome"),
            P("samples", None),
            P("genome"),
            P(),
            P(("genome", "samples")),
            P(("genome", "samples")),
        ),
        out_specs=(P(("genome", "samples"), None), P(("genome", "samples"), None)),
        check_vma=False,
    )
```

```python
import jax
import jax.numpy as jnp
from jax import lax
from jax.experimental import pallas as pl
from jax.experimental.pallas import tpu as pltpu
from jax.sharding import PartitionSpec as P


F32, BF16 = jnp.float32, jnp.bfloat16
NT = (((1,), (1,)), ((), ()))
NN = (((1,), (0,)), ((), ()))
LANES = 128
SUBLANES = 8
VMEM_LIMIT = 16 * 2**20


def rounded(size, unit):
    return (size + unit - 1) // unit * unit


def visit_order(groups):
    masks, bit = [0], groups // 2
    while bit:
        masks = [mask | bit for mask in masks] + masks
        bit //= 2
    return masks


def split(x):
    high = x.astype(BF16)
    rest = x - high.astype(F32)
    middle = rest.astype(BF16)
    return high, middle, (rest - middle.astype(F32)).astype(BF16)


def exact_dot(a, b, dims):
    return sum(lax.dot_general(a, part, dims, preferred_element_type=F32) for part in split(b))


def exact_dot_left(a, b, dims):
    return sum(lax.dot_general(part, b, dims, preferred_element_type=F32) for part in split(a))


def first_kernel(total_samples, groups):
    def body(
        weight_hbm, genotypes, residuals_hbm, classes_hbm, send, keep,
        buffer, sums, sems, class_weight, residuals, classes, small_sems,
    ):
        phenos, rows = residuals.shape
        share = send.shape[2]
        columns = groups * share
        me = lax.axis_index("samples")
        extra = send.shape[1] - phenos
        steps = sems.shape[0]
        piece = rows // steps
        small_copies = [
            pltpu.make_async_copy(source, target, small_sems.at[k])
            for k, (source, target) in enumerate(
                [(residuals_hbm, residuals), (classes_hbm, classes), (weight_hbm, class_weight)]
            )
        ]
        copies = [
            pltpu.make_async_copy(
                genotypes.at[pl.ds(k * piece, piece), :],
                buffer.at[pl.ds(k * piece, piece), :],
                sems.at[k],
            )
            for k in range(steps)
        ]
        for each in small_copies + copies:
            each.start()
        for each in small_copies:
            each.wait()
        squares = jnp.square(residuals[...].astype(F32))
        spread = exact_dot(jnp.ones((extra, rows), BF16), squares, NT)
        kind = classes[...].reshape(1, columns)
        weight = jnp.zeros((1, columns), F32)
        for c in range(class_weight.shape[0]):
            weight = jnp.where(kind == c, class_weight[c], weight)
        for k in range(steps):
            copies[k].wait()
            spot = pl.ds(k * piece, piece)
            dosage = buffer[spot, :].astype(F32)
            part = lax.dot_general(
                residuals[:, spot], dosage.astype(BF16), NN, preferred_element_type=F32
            )
            counts = jnp.sum((dosage * dosage).reshape(-1, SUBLANES, columns), axis=0)
            if k:
                part, counts = part + sums[:phenos], counts + sums[phenos:]
            if k < steps - 1:
                sums[:phenos], sums[phenos:] = part, counts
        scores = part * (weight * total_samples ** (-0.5))
        quad = (weight * weight / total_samples) * jnp.sum(counts, axis=0, keepdims=True)
        both = jnp.concatenate([scores, jnp.broadcast_to(quad, (extra, columns))], axis=0)
        folded = []
        for c in range(groups):
            lanes = [
                both[:, c * share + b : c * share + b + LANES] for b in range(0, share, LANES)
            ]
            folded.append(sum(lanes[1:], lanes[0]))
        folded = jnp.concatenate(folded, axis=1)
        shape = (extra, groups * LANES)
        mark = lax.broadcasted_iota(jnp.int32, shape, 1) // LANES + 1
        mark = (mark == lax.broadcasted_iota(jnp.int32, shape, 0)).astype(F32).astype(BF16)
        totals = exact_dot(mark, folded, NT)
        row_of = lax.broadcasted_iota(jnp.int32, (extra, LANES), 0)
        small = jnp.concatenate([totals, jnp.zeros((extra, LANES - phenos - extra), F32)], axis=1)
        spread = jnp.concatenate([spread, jnp.zeros((extra, LANES - phenos), F32)], axis=1)
        small = jnp.where(row_of == groups + 1, spread, small)
        below = jnp.where(lax.broadcasted_iota(jnp.int32, (extra, columns), 0) == 0, quad, 0.0)
        for c in range(groups):
            for out, slot, is_here in places(send, keep, me ^ c, groups):

                @pl.when(is_here)
                def _():
                    part_of = slice(c * share, (c + 1) * share)
                    out[slot, :phenos, :] = scores[:, part_of]
                    out[slot, phenos:, :] = below[:, part_of]

        for out in (send, keep):
            out[0, phenos:, :LANES] += small

    return body


def places(send, keep, mask, groups):
    order = visit_order(groups)
    half = groups // 2
    slot = sum(
        jnp.where(mask == order[k], k % half, 0) for k in range(groups)
    )
    return [(send, slot, mask % 2 == 1), (keep, slot, mask % 2 == 0)]


def first_variant(real_share):
    groups = lax.axis_size("samples")
    return (lax.axis_index("genome") * groups + lax.axis_index("samples")) * real_share


def second_kernel(real_share):
    def body(start_ref, end_ref, block, totals, prefix, own_genes, mask):
        phenos, share = prefix.shape
        genes = own_genes.shape[0]
        me = lax.axis_index("samples")
        rows = lax.broadcasted_iota(jnp.int32, (share, share), 0)
        cols = lax.broadcasted_iota(jnp.int32, (share, share), 1)
        upper = (rows <= cols).astype(F32).astype(BF16)
        small = totals[...]
        row_of = lax.broadcasted_iota(jnp.int32, small.shape, 0)
        earlier = jnp.sum(
            jnp.where((row_of >= 1) & (row_of < me + 1), small, 0.0), axis=0, keepdims=True
        )
        inner = exact_dot_left(block[:phenos], upper, NN)
        prefix[...] = inner + column(earlier, phenos)
        base = first_variant(real_share)
        inside = window_mask(start_ref, end_ref, base, genes, share)
        own_genes[...] = exact_dot(inside.astype(BF16), block[...], NT)
        mask[...] = window_mask(start_ref, end_ref, base - real_share, genes, share)

    return body


def column(row, size):
    return jnp.transpose(jnp.broadcast_to(row, (SUBLANES, LANES)))[:size, :1]


def window_mask(start_ref, end_ref, base, genes, share):
    index = lax.broadcasted_iota(jnp.int32, (genes, 1), 0)
    start = jnp.zeros((genes, 1), jnp.int32)
    end = jnp.zeros((genes, 1), jnp.int32)
    for g in range(genes):
        start = jnp.where(index == g, start_ref[g] - base, start)
        end = jnp.where(index == g, end_ref[g] - base, end)
    spot = lax.broadcasted_iota(jnp.int32, (genes, share), 1)
    return ((spot >= start) & (spot < end)).astype(F32)


def last_kernel(total_samples, total_vars, groups):
    def body(prefix, carry, totals, near, far, own_genes, mask, track, stat):
        phenos = prefix.shape[0]
        track[...] = (prefix[...] + column(carry[...], phenos)) * total_vars ** (-0.5)
        odd = lax.axis_index("samples") % 2 == 1
        earlier = jnp.where(odd, near[...], far[...])
        sums = own_genes[...] + exact_dot(mask[...].astype(BF16), earlier, NT)
        variance = totals[groups + 1 : groups + 2, :phenos] / total_samples + 1e-05
        quad = sums[:, phenos : phenos + 1]
        stat[...] = jnp.square(sums[:, :phenos]) / (variance * (quad + 1.0))

    return body


def call(body, ins, outs, final=False, **more):
    spaces = {"s": pltpu.SMEM, "v": pltpu.VMEM, "h": pltpu.HBM}
    args = [
        x if kind == "s" else pltpu.with_memory_space_constraint(x, spaces[kind])
        for kind, x in ins
    ]
    result = jax.ShapeDtypeStruct if final else pltpu.VMEM
    return pl.pallas_call(
        body,
        in_specs=[pl.BlockSpec(memory_space=spaces[kind]) for kind, _ in ins],
        out_specs=[pl.BlockSpec(memory_space=pltpu.VMEM)] * len(outs),
        out_shape=[result(shape, F32) for shape in outs],
        compiler_params=pltpu.CompilerParams(vmem_limit_bytes=VMEM_LIMIT),
        **more,
    )(*args)


def block_prefix(whole, blocks, groups):
    devices = blocks * groups
    index = lax.axis_index("genome")
    both_axes = ("genome", "samples")

    def exchange(x, mask):
        return lax.ppermute(x, both_axes, [(k, k ^ mask ^ 1) for k in range(devices)])

    carry = jnp.zeros_like(whole)
    bit = 1
    while bit < blocks:
        other = exchange(whole, bit * groups)
        carry = carry + jnp.where((index & bit) != 0, other, 0.0)
        whole = whole + other
        bit *= 2
    bit = 2
    while bit < groups:
        carry = carry + exchange(carry, bit)
        bit *= 2
    return carry


def local(genotypes, residuals, variant_class, class_weight, gene_start, gene_end):
    groups = lax.axis_size("samples")
    blocks = lax.axis_size("genome")
    both_axes = ("genome", "samples")
    sample_rows, block_vars = genotypes.shape
    phenos = residuals.shape[1]
    genes = gene_start.shape[0]
    real_share = block_vars // groups
    share = rounded(real_share, LANES)
    total_samples = sample_rows * groups
    total_vars = block_vars * blocks
    extra = rounded(groups + 2, SUBLANES)
    rows = phenos + extra
    devices = groups * blocks
    half = groups // 2
    classes = variant_class
    if share != real_share:
        missing = share - real_share
        classes = jnp.pad(variant_class.reshape(groups, real_share), ((0, 0), (0, missing)))
        classes = classes.reshape(groups * share)
        genotypes = jnp.pad(
            genotypes.reshape(sample_rows, groups, real_share), ((0, 0), (0, 0), (0, missing))
        ).reshape(sample_rows, groups * share)

    send, keep = call(
        first_kernel(total_samples, groups),
        [("h", class_weight), ("h", genotypes), ("h", residuals.T), ("h", classes)],
        [(half, rows, share)] * 2,
        scratch_shapes=[
            pltpu.VMEM((sample_rows, groups * share), jnp.int32),
            pltpu.VMEM((phenos + SUBLANES, groups * share), F32),
            pltpu.SemaphoreType.DMA((4,)),
            pltpu.SMEM(class_weight.shape, F32),
            pltpu.VMEM((phenos, sample_rows), BF16),
            pltpu.VMEM((groups * share,), jnp.int32),
            pltpu.SemaphoreType.DMA((3,)),
        ],
    )

    bit = 1
    pair = keep + lax.ppermute(send, "samples", [(i, i ^ bit) for i in range(groups)])
    while half > 2:
        bit, half = 2 * bit, half // 2
        small = jnp.pad(
            pair[:1, phenos + 1 :, :LANES], ((0, half - 1), (phenos + 1, 0), (0, share - LANES))
        )
        other = lax.ppermute(pair[:half], "samples", [(i, i ^ bit) for i in range(groups)])
        pair = pair[half:] + other + small
    mine = pair[0, phenos:, :LANES]
    whole = jnp.sum(mine[1 : groups + 1], axis=0, keepdims=True)
    carry = block_prefix(whole, blocks, groups)
    bit *= 2
    received = lax.ppermute(pair[0], "samples", [(i, i ^ bit) for i in range(groups)])

    block = pair[1] + received
    totals = mine + received[phenos:, :LANES]
    near = lax.ppermute(block, both_axes, [(k, k ^ 1) for k in range(devices)])
    far = lax.ppermute(block, both_axes, [(k, k + 1) for k in range(1, devices - 1, 2)])
    prefix, own_genes, mask = call(
        second_kernel(real_share),
        [("s", gene_start), ("s", gene_end), ("v", block), ("v", totals)],
        [(phenos, share), (genes, rows), (genes, share)],
    )
    track, stat = call(
        last_kernel(total_samples, total_vars, groups),
        [("v", x) for x in (prefix, carry, totals, near, far, own_genes, mask)],
        [(phenos, share), (genes, phenos)],
        final=True,
    )
    return track[:, :real_share].T, stat


def solution(mesh):
    return jax.shard_map(
        local,
        mesh=mesh,
        in_specs=(
            P("samples", "genome"),
            P("samples", None),
            P("genome"),
            P(),
            P(("genome", "samples")),
            P(("genome", "samples")),
        ),
        out_specs=(P(("genome", "samples"), None), P(("genome", "samples"), None)),
        check_vma=False,
    )
```
